256 devices in a mesh: row: 64 (over z, y, core), col: 4 (over x).
Axes of the slice: x: 4, y: 4, z: 8, core: 2. Of those that a mesh axis runs over, the one named last changes fastest.
Arguments:
- node_feat: bfloat16 [131072, 50], P(('row', 'col'))
- w_one: float32 [50, 2048], replicated
- w_two: float32 [2048, 121], replicated
- send_rows: int32 [1024, 8], P(('row', 'col'))
- edge_src: int32 [131072, 12], P(('row', 'col'))
- edge_wt: float32 [131072, 12], P(('row', 'col'))
- labels: int32 [131072], P(('row', 'col'))
- label_mask: int32 [131072], P(('row', 'col'))
Outputs:
- output 1: float32 [], replicated
- output 2: float32 [50, 2048], replicated
- output 3: float32 [2048, 121], replicated
All inputs are finite; a program needn't handle non-finite values.
Results may differ from the reference program's by a relative error of at most 0.001.
Values are sent between devices in bfloat16 or wider.
A program may use at most 768 MiB of HBM per device.

```python
import jax
import jax.numpy as jnp
from jax import lax

GRID_ROWS = 64
GRID_COLS = 4
NODES_DEV = 512
HALO_ROWS = 8
DEGREE = 12
FEAT_IN = 50
FEAT_HID = 2048
CLASSES = 121
PEERS = 4


def setup_inputs(seed: int = 0) -> dict:
    n_devices = GRID_ROWS * GRID_COLS
    n_nodes = n_devices * NODES_DEV
    key_list = jax.random.split(jax.random.key(seed), 12)
    node_feat = jax.random.normal(key_list[0], (n_nodes, FEAT_IN), jnp.float32).astype(jnp.bfloat16)
    w_one = jax.random.normal(key_list[1], (FEAT_IN, FEAT_HID), jnp.float32) * FEAT_IN ** -0.5
    w_two = jax.random.normal(key_list[2], (FEAT_HID, CLASSES), jnp.float32) * FEAT_HID ** -0.5
    send_rows = jax.random.randint(key_list[3], (n_devices * PEERS, HALO_ROWS), 0, NODES_DEV)
    own_src = jax.random.randint(key_list[4], (n_nodes, DEGREE), 0, NODES_DEV)
    halo_src = jax.random.randint(key_list[5], (n_nodes, DEGREE), NODES_DEV, NODES_DEV + PEERS * HALO_ROWS)
    forced_pos = jax.random.randint(key_list[6], (n_nodes, 1), 0, DEGREE)
    coin_draw = jax.random.randint(key_list[7], (n_nodes, DEGREE), 0, 8)
    is_cut = (coin_draw == 0) | (jnp.arange(DEGREE)[None, :] == forced_pos)
    edge_src = jnp.where(is_cut, halo_src, own_src)
    raw_wt = jax.random.uniform(key_list[8], (n_nodes, DEGREE), jnp.float32, 0.5, 1.5)
    edge_wt = raw_wt * lax.rsqrt(jnp.sum(raw_wt * raw_wt, axis=1, keepdims=True))
    labels = jax.random.randint(key_list[9], (n_nodes,), 0, CLASSES)
    mask_draw = jax.random.randint(key_list[10], (n_nodes,), 0, 2)
    label_mask = jnp.where(jnp.arange(n_nodes) % NODES_DEV == 0, 1, mask_draw)
    return {"node_feat": node_feat, "w_one": w_one, "w_two": w_two, "send_rows": send_rows,
            "edge_src": edge_src, "edge_wt": edge_wt, "labels": labels, "label_mask": label_mask}


def extended_globals(send_rows):
    n_devices = GRID_ROWS * GRID_COLS
    list_table = send_rows.reshape(n_devices, PEERS, HALO_ROWS)
    dev_ids = jnp.arange(n_devices)
    row_id = dev_ids // GRID_COLS
    col_id = dev_ids % GRID_COLS
    peer_dev = jnp.stack([
        row_id * GRID_COLS + (col_id - 1) % GRID_COLS,
        row_id * GRID_COLS + (col_id + 1) % GRID_COLS,
        ((row_id - 1) % GRID_ROWS) * GRID_COLS + col_id,
        ((row_id + 1) % GRID_ROWS) * GRID_COLS + col_id], axis=1)
    back_slot = jnp.array([1, 0, 3, 2])
    halo_rows = peer_dev[:, :, None] * NODES_DEV + list_table[peer_dev, back_slot[None, :], :]
    own_rows = dev_ids[:, None] * NODES_DEV + jnp.arange(NODES_DEV)[None, :]
    return jnp.concatenate([own_rows, halo_rows.reshape(n_devices, PEERS * HALO_ROWS)], axis=1)


def global_src(send_rows, edge_src):
    n_devices = GRID_ROWS * GRID_COLS
    ext_global = extended_globals(send_rows)
    local_src = edge_src.reshape(n_devices, NODES_DEV * DEGREE)
    return jnp.take_along_axis(ext_global, local_src, axis=1).reshape(n_devices * NODES_DEV, DEGREE)


def aggregate(table, gidx, edge_wt):
    def add_edge(total, cols):
        idx_col, wt_col = cols
        return total + wt_col[:, None] * table[idx_col].astype(jnp.float32), None
    start_acc = jnp.zeros((gidx.shape[0], table.shape[1]), jnp.float32)
    result, _ = lax.scan(add_edge, start_acc, (gidx.T, edge_wt.T))
    return result


def scatter_back(grad, gidx, edge_wt):
    def add_edge(total, cols):
        idx_col, wt_col = cols
        return total.at[idx_col].add(wt_col[:, None] * grad), None
    start_acc = jnp.zeros(grad.shape, jnp.float32)
    result, _ = lax.scan(add_edge, start_acc, (gidx.T, edge_wt.T))
    return result


def reference(node_feat, w_one, w_two, send_rows, edge_src, edge_wt, labels, label_mask):
    gidx = global_src(send_rows, edge_src)
    w_one_b = w_one.astype(jnp.bfloat16)
    w_two_b = w_two.astype(jnp.bfloat16)
    z_one = aggregate(node_feat, gidx, edge_wt).astype(jnp.bfloat16)
    h_one = jnp.maximum(jnp.dot(z_one, w_one_b, preferred_element_type=jnp.float32), 0.0).astype(jnp.bfloat16)
    z_two = aggregate(h_one, gidx, edge_wt).astype(jnp.bfloat16)
    logits = jnp.dot(z_two, w_two_b, preferred_element_type=jnp.float32)
    weight = label_mask.astype(jnp.float32)
    label_count = jnp.sum(weight)
    log_norm = jax.nn.logsumexp(logits, axis=1)
    picked = jnp.take_along_axis(logits, labels[:, None], axis=1)[:, 0]
    mean_loss = jnp.sum(weight * (log_norm - picked)) / label_count
    class_prob = jnp.exp(logits - log_norm[:, None])
    onehot = (jnp.arange(CLASSES)[None, :] == labels[:, None]).astype(jnp.float32)
    d_logits = ((class_prob - onehot) * (weight / label_count)[:, None]).astype(jnp.bfloat16)
    grad_two = jnp.dot(z_two.T, d_logits, preferred_element_type=jnp.float32)
    d_z_two = jnp.dot(d_logits, w_two_b.T, preferred_element_type=jnp.float32)
    d_h_one = scatter_back(d_z_two, gidx, edge_wt)
    d_y_one = jnp.where(h_one > 0, d_h_one, 0.0).astype(jnp.bfloat16)
    grad_one = jnp.dot(z_one.T, d_y_one, preferred_element_type=jnp.float32)
    return (mean_loss, grad_one, grad_two)
```

```python
import functools

import jax
import jax.numpy as jnp
from jax import lax
from jax.experimental import pallas as pl
from jax.experimental.pallas import tpu as pltpu
from jax.sharding import PartitionSpec as P

F32 = jnp.float32
BF16 = jnp.bfloat16
MESH = pl.DeviceIdType.MESH
LANES = 128
PEERS = 4


def mm(a, b, ca, cb):
    return lax.dot_general(a, b, (((ca,), (cb,)), ((), ())), preferred_element_type=F32)


def split3(v):
    hi = v.astype(BF16)
    rest = v - hi.astype(F32)
    mid = rest.astype(BF16)
    low = (rest - mid.astype(F32)).astype(BF16)
    return hi, mid, low


class Grid:
    def __init__(self, dims):
        self.nx, self.ny, self.nz, self.nc = dims
        self.row = lax.axis_index('row')
        self.x = lax.axis_index('col')
        self.c = lax.rem(self.row, self.nc)
        self.y = lax.rem(self.row // self.nc, self.ny)
        self.z = self.row // (self.nc * self.ny)
        self.n_rows = self.nz * self.ny * self.nc

    def size(self, axis):
        return {'x': self.nx, 'y': self.ny, 'z': self.nz, 'c': self.nc}[axis]

    def pos(self, axis):
        return getattr(self, axis)

    def plus(self, axis, d):
        n = self.size(axis)
        return lax.rem(self.pos(axis) + d, n)

    def dev(self, axis, d):
        at = {'x': self.x, 'y': self.y, 'z': self.z, 'c': self.c}
        at[axis] = self.plus(axis, d)
        return ((at['z'] * self.ny + at['y']) * self.nc + at['c'], at['x'])

    def peer(self, p):
        if p == 0:
            return (self.row, lax.rem(self.x + self.nx - 1, self.nx))
        if p == 1:
            return (self.row, lax.rem(self.x + 1, self.nx))
        if p == 2:
            return (lax.rem(self.row + self.n_rows - 1, self.n_rows), self.x)
        return (lax.rem(self.row + 1, self.n_rows), self.x)


class Stream:
    def __init__(self, g, refs, rows):
        (self.b, self.rc, self.h, self.r1, self.p, self.r2, self.q, self.rz,
         self.f, self.ssem, self.rsem) = refs
        self.g, self.rows = g, rows
        self.n_sem = 0
        self.sent = []

    def copy(self, src, dst, dev):
        k = self.n_sem
        self.n_sem += 1
        op = pltpu.make_async_remote_copy(src_ref=src, dst_ref=dst, send_sem=self.ssem.at[k],
                                          recv_sem=self.rsem.at[k], device_id=dev, device_id_type=MESH)
        op.start()
        self.sent.append(op)
        return op

    def steps(self):
        g, rows = self.g, self.rows
        half, quarter = rows // 2, rows // 4
        ds = lambda start, size: pl.ds(pl.multiple_of(start, size), size)
        orders = (('x', 'y'), ('y', 'x'))
        other = g.plus('c', 1)
        op = self.copy(self.b.at[ds(other * half, half)], self.rc, g.dev('c', 1))
        yield
        op.wait_recv()
        self.h[...] = self.b[ds(g.c * half, half)] + self.rc[...]
        n1 = quarter // g.nx
        ops = []
        for col, (a1, a2) in enumerate(orders):
            for d in range(1, g.size(a1)):
                ops.append(self.copy(self.h.at[ds(col * quarter + g.plus(a1, d) * n1, n1)],
                                     self.r1.at[col, d - 1], g.dev(a1, d)))
        yield
        for op in ops:
            op.wait_recv()
        for col, (a1, a2) in enumerate(orders):
            total = self.h[ds(col * quarter + g.pos(a1) * n1, n1)]
            for d in range(1, g.size(a1)):
                total = total + self.r1[col, d - 1]
            self.p[col] = total
        n2 = n1 // g.ny
        ops = []
        for col, (a1, a2) in enumerate(orders):
            for d in range(1, g.size(a2)):
                ops.append(self.copy(self.p.at[col, ds(g.plus(a2, d) * n2, n2)],
                                     self.r2.at[col, d - 1], g.dev(a2, d)))
        yield
        for op in ops:
            op.wait_recv()
        for col, (a1, a2) in enumerate(orders):
            total = self.p[col, ds(g.pos(a2) * n2, n2)]
            for d in range(1, g.size(a2)):
                total = total + self.r2[col, d - 1]
            self.q[pl.ds(col * n2, n2)] = total
        n3 = 2 * n2 // g.nz
        ops = []
        for d in range(1, g.nz):
            ops.append(self.copy(self.q.at[ds(g.plus('z', d) * n3, n3)], self.rz.at[d - 1], g.dev('z', d)))
        yield
        for op in ops:
            op.wait_recv()
        total = self.q[ds(g.z * n3, n3)]
        for d in range(1, g.nz):
            total = total + self.rz[d - 1]
        base1 = [g.c * half + col * quarter for col in range(2)]
        base2 = [base1[0] + g.x * n1, base1[1] + g.y * n1]
        base3 = [base2[0] + g.y * n2, base2[1] + g.x * n2]
        per_col = g.nz // 2
        which = g.z // per_col
        start = base3[0] * (1 - which) + base3[1] * which + lax.rem(g.z, per_col) * n3
        self.f[ds(start, n3)] = total
        ops = []
        for d in range(1, g.nz):
            ops.append(self.copy(self.f.at[ds(start, n3)], self.f.at[ds(start, n3)], g.dev('z', d)))
        yield
        for op in ops:
            op.wait_recv()
        ops = []
        for col, (a1, a2) in enumerate(orders):
            for d in range(1, g.size(a2)):
                part = self.f.at[ds(base3[col], n2)]
                ops.append(self.copy(part, part, g.dev(a2, d)))
        yield
        for op in ops:
            op.wait_recv()
        ops = []
        for col, (a1, a2) in enumerate(orders):
            for d in range(1, g.size(a1)):
                part = self.f.at[ds(base2[col], n1)]
                ops.append(self.copy(part, part, g.dev(a1, d)))
        yield
        for op in ops:
            op.wait_recv()
        part = self.f.at[ds(g.c * half, half)]
        op = self.copy(part, part, g.dev('c', 1))
        yield
        op.wait_recv()
        for op in self.sent:
            op.wait_send()


def step_kernel(dims, feat_in, classes, feat_ref, w1_ref, w2_ref, send_ref, src_ref, wt_ref, lab_ref, mask_ref,
                loss_ref, g1_ref, g2_ref, *scratch):
    (at, fp, w1p, w2p, sel, z1t, z1tb, h1t, h1h, z2t, d1t, ptc,
     hs, hr, hs_sem, hr_sem, mb, mr, ms_sem, mr_sem) = scratch[:20]
    refs2, refs1 = scratch[20:31], scratch[31:42]
    g = Grid(dims)
    n = feat_ref.shape[1]
    hid = w1_ref.shape[1]
    halo = send_ref.shape[0] * send_ref.shape[1]
    per = send_ref.shape[1]
    deg = src_ref.shape[0]
    ext = n + halo

    barrier = pltpu.get_barrier_semaphore()
    greet = [g.dev('c', 1)]
    for axis in ('x', 'y', 'z'):
        greet += [g.dev(axis, d) for d in range(1, g.size(axis))]
    far = lax.rem(g.row + g.n_rows + 2 * g.c - 1, g.n_rows)
    greet.append((far, g.x))
    for dev in greet:
        pl.semaphore_signal(barrier, inc=1, device_id=dev, device_id_type=MESH)

    weight = mask_ref[...].astype(F32)
    mb[0] = jnp.full(mb.shape[1:], 1.0, F32) * jnp.sum(weight)

    def build(i, carry):
        first = pl.multiple_of(i * 16, 16)
        ids = first + lax.broadcasted_iota(jnp.int32, (16, n), 0)
        total = jnp.zeros((16, n), F32)
        for k in range(deg):
            total = total + jnp.where(src_ref[k:k + 1, :] == ids, wt_ref[k:k + 1, :], 0.0)
        parts = split3(total)
        for j in range(3):
            at[j, pl.ds(first, 16), :] = parts[j]
        return carry

    lax.fori_loop(0, ext // 16, build, 0)

    eye = lax.broadcasted_iota(jnp.int32, (per, per), 0) == lax.broadcasted_iota(jnp.int32, (per, per), 1)
    lane_ids = lax.broadcasted_iota(jnp.int32, (per, n), 1)
    picks = []
    for p in range(PEERS):
        rows = jnp.broadcast_to(send_ref[p:p + 1, :], (per, per))
        column = jnp.sum(jnp.where(eye, rows, 0), axis=1, keepdims=True)
        picks.append((column == lane_ids).astype(F32))
    sel[...] = jnp.concatenate(picks, axis=0).astype(BF16)

    fp[...] = jnp.concatenate([feat_ref[...].astype(F32), jnp.zeros((LANES - feat_in, n), F32)], axis=0).astype(BF16)
    w1p[...] = jnp.concatenate([w1_ref[...], jnp.zeros((w1p.shape[0] - feat_in, hid), F32)], axis=0).astype(BF16)
    w2p[...] = jnp.concatenate([w2_ref[...], jnp.zeros((hid, LANES - classes), F32)], axis=1).astype(BF16)

    pl.semaphore_wait(barrier, len(greet))

    def exchange(stage, rows):
        hs[stage] = rows
        ops = []
        for p in range(PEERS):
            ops.append(pltpu.make_async_remote_copy(
                src_ref=hs.at[stage, pl.ds(p * per, per)], dst_ref=hr.at[stage, pl.ds((p ^ 1) * per, per)],
                send_sem=hs_sem.at[stage, p], recv_sem=hr_sem.at[stage, p ^ 1],
                device_id=g.peer(p), device_id_type=MESH))
            ops[-1].start()
        return ops

    def arrived(ops):
        for op in ops:
            op.wait()

    def count_steps():
        k = 0
        for stage, axis in enumerate(('c', 'x', 'y', 'z')):
            ops = []
            for d in range(1, g.size(axis)):
                ops.append(pltpu.make_async_remote_copy(
                    src_ref=mb.at[stage], dst_ref=mr.at[k], send_sem=ms_sem.at[k], recv_sem=mr_sem.at[k],
                    device_id=g.dev(axis, d), device_id_type=MESH))
                ops[-1].start()
                k += 1
            yield
            arrived(ops)
            total = mb[stage]
            for j in range(k - len(ops), k):
                total = total + mr[j]
            mb[stage + 1] = total

    count = count_steps()
    ops = exchange(0, mm(sel[...], fp[...], 1, 1))
    next(count)

    z1 = mm(fp[...], at[0, 0:n, :], 1, 0) + mm(fp[...], at[1, 0:n, :], 1, 0) + mm(fp[...], at[2, 0:n, :], 1, 0)
    arrived(ops)
    fh = hr[0].astype(BF16)
    z1 = z1 + (mm(fh, at[0, n:ext, :], 0, 0) + mm(fh, at[1, n:ext, :], 0, 0) + mm(fh, at[2, n:ext, :], 0, 0))
    z1t[...] = z1.astype(BF16)
    ops = exchange(1, mm(sel[...], z1t[...], 1, 1))
    next(count)
    kf = w1p.shape[0]
    chunk = min(hid, 512)
    n_chunks = hid // chunk
    for i in range(n_chunks):
        s = slice(i * chunk, (i + 1) * chunk)
        h1t[s, :] = jnp.maximum(mm(w1p[:, s], z1t[0:kf, :], 0, 0), 0.0).astype(BF16)
    next(count)
    z1tb[0:LANES // 2, :] = jnp.zeros((LANES // 2, n), BF16)
    z1tb[LANES // 2:, :] = z1t[0:LANES // 2, :]

    def own_part(i):
        s = slice(i * chunk, (i + 1) * chunk)
        return mm(h1t[s, :], at[0, 0:n, :], 1, 0) + mm(h1t[s, :], at[1, 0:n, :], 1, 0) + mm(h1t[s, :], at[2, 0:n, :], 1, 0)

    first_part = own_part(0)
    arrived(ops)
    z1h = hr[1][:, 0:kf].astype(BF16)
    for i in range(n_chunks):
        s = slice(i * chunk, (i + 1) * chunk)
        h1h[s, :] = jnp.maximum(mm(w1p[:, s], z1h, 0, 1), 0.0).astype(BF16)
    logits = jnp.zeros((LANES, n), F32)
    for i in range(n_chunks):
        s = slice(i * chunk, (i + 1) * chunk)
        part = first_part if i == 0 else own_part(i)
        hh = h1h[s, :]
        part = part + (mm(hh, at[0, n:ext, :], 1, 0) + mm(hh, at[1, n:ext, :], 1, 0) + mm(hh, at[2, n:ext, :], 1, 0))
        z2 = part.astype(BF16)
        z2t[s, :] = z2
        logits = logits + mm(w2p[s, :], z2, 0, 0)
        if i == n_chunks // 2:
            next(count)
    for _ in count:
        pass

    label_count = mb[4, 0:1, 0:1]
    ids = lax.broadcasted_iota(jnp.int32, (LANES, n), 0)
    valid = ids < classes
    top = jnp.max(jnp.where(valid, logits, -jnp.inf), axis=0, keepdims=True)
    log_norm = jnp.log(jnp.sum(jnp.where(valid, jnp.exp(logits - top), 0.0), axis=0, keepdims=True)) + top
    onehot = ids == lab_ref[...]
    picked = jnp.sum(jnp.where(onehot, logits, 0.0), axis=0, keepdims=True)
    loss = jnp.sum(weight * (log_norm - picked))
    prob = jnp.exp(logits - log_norm)
    scale = weight / label_count
    gt = jnp.where(valid, (prob - onehot.astype(F32)) * scale, 0.0).astype(BF16)

    ops = exchange(2, mm(at[0, n:ext, :], gt, 1, 1) + mm(at[1, n:ext, :], gt, 1, 1) + mm(at[2, n:ext, :], gt, 1, 1))

    b2 = refs2[0]
    lane = lax.broadcasted_iota(jnp.int32, (chunk, LANES), 1)
    for i in range(n_chunks):
        s = slice(i * chunk, (i + 1) * chunk)
        b2[s, :] = jnp.where(lane == classes, loss, mm(z2t[s, :], gt, 1, 1))
    stream2 = Stream(g, refs2, hid).steps()
    next(stream2)

    pt = mm(gt, at[0, 0:n, :], 1, 1) + mm(gt, at[1, 0:n, :], 1, 1) + mm(gt, at[2, 0:n, :], 1, 1)
    arrived(ops)
    for part in split3(hr[2]):
        pt = pt + mm(part, sel[...], 0, 0)
    for j, part in enumerate(split3(pt)):
        ptc[j] = part
    next(stream2)
    for i in range(n_chunks):
        s = slice(i * chunk, (i + 1) * chunk)
        dh = mm(w2p[s, :], ptc[0], 1, 0) + mm(w2p[s, :], ptc[1], 1, 0) + mm(w2p[s, :], ptc[2], 1, 0)
        d1t[s, :] = jnp.where(h1t[s, :].astype(F32) > 0.0, dh, 0.0).astype(BF16)
    next(stream2)
    b1 = refs1[0]
    half = hid // 2
    b1[...] = mm(d1t[0:half, :], z1t[...], 1, 1) + mm(d1t[half:hid, :], z1tb[...], 1, 1)
    stream1 = Stream(g, refs1, half).steps()
    next(stream1)
    active = [stream2, stream1]
    while active:
        for stream in list(active):
            if next(stream, 'end') == 'end':
                active.remove(stream)

    f2, f1 = refs2[8], refs1[8]
    loss_ref[...] = f2[0:1, classes:classes + 1] / label_count
    g2_ref[...] = f2[:, 0:classes]
    flip = jnp.transpose(f1[...])
    g1_ref[:, 0:half] = flip[0:feat_in, :]
    g1_ref[:, half:hid] = flip[LANES // 2:LANES // 2 + feat_in, :]


def stream_scratch(rows, dims):
    nx, ny, nz, nc = dims
    half, quarter = rows // 2, rows // 4
    n1 = quarter // nx
    n2 = n1 // ny
    n3 = 2 * n2 // nz
    copies = 2 + 4 * (nx - 1) + 4 * (ny - 1) + 2 * (nz - 1)
    return [
        pltpu.VMEM((rows, LANES), F32), pltpu.VMEM((half, LANES), F32), pltpu.VMEM((half, LANES), F32),
        pltpu.VMEM((2, nx - 1, n1, LANES), F32), pltpu.VMEM((2, n1, LANES), F32),
        pltpu.VMEM((2, ny - 1, n2, LANES), F32), pltpu.VMEM((2 * n2, LANES), F32),
        pltpu.VMEM((nz - 1, n3, LANES), F32), pltpu.VMEM((rows, LANES), F32),
        pltpu.SemaphoreType.DMA((copies,)), pltpu.SemaphoreType.DMA((copies,))]


def make_step(dims):
    def device_step(node_feat, w_one, w_two, send_rows, edge_src, edge_wt, labels, label_mask):
        n, feat_in = node_feat.shape
        hid, classes = w_two.shape
        halo = send_rows.size
        ext = n + halo
        nx, ny, nz, nc = dims
        n_count = nx + ny + nz + nc - 4
        kf = 64
        scratch = [
            pltpu.VMEM((3, ext, n), BF16), pltpu.VMEM((LANES, n), BF16), pltpu.VMEM((kf, hid), BF16), pltpu.VMEM((hid, LANES), BF16),
            pltpu.VMEM((halo, n), BF16), pltpu.VMEM((LANES, n), BF16), pltpu.VMEM((LANES, n), BF16),
            pltpu.VMEM((hid, n), BF16), pltpu.VMEM((hid, halo), BF16), pltpu.VMEM((hid, n), BF16),
            pltpu.VMEM((hid, n), BF16), pltpu.VMEM((3, LANES, n), BF16),
            pltpu.VMEM((3, halo, LANES), F32), pltpu.VMEM((3, halo, LANES), F32),
            pltpu.SemaphoreType.DMA((3, PEERS)), pltpu.SemaphoreType.DMA((3, PEERS)),
            pltpu.VMEM((5, 8, LANES), F32), pltpu.VMEM((n_count, 8, LANES), F32),
            pltpu.SemaphoreType.DMA((n_count,)), pltpu.SemaphoreType.DMA((n_count,)),
        ] + stream_scratch(hid, dims) + stream_scratch(hid // 2, dims)
        vmem = pl.BlockSpec(memory_space=pltpu.VMEM)
        loss, grad_one, grad_two = pl.pallas_call(
            functools.partial(step_kernel, dims, feat_in, classes),
            out_shape=(jax.ShapeDtypeStruct((1, 1), F32), jax.ShapeDtypeStruct((feat_in, hid), F32),
                       jax.ShapeDtypeStruct((hid, classes), F32)),
            in_specs=[vmem] * 8, out_specs=(vmem,) * 3, scratch_shapes=scratch,
            compiler_params=pltpu.CompilerParams(collective_id=0, has_side_effects=True,
                                                 vmem_limit_bytes=60 * 1024 * 1024),
        )(node_feat.T, w_one, w_two, send_rows, edge_src.T, edge_wt.T, labels.reshape(1, n), label_mask.reshape(1, n))
        return loss[0, 0], grad_one, grad_two
    return device_step


def build(mesh, dims):
    grid_axes = ('row', 'col')
    rows_spec = P(grid_axes, None)
    vec_spec = P(grid_axes)
    return jax.shard_map(make_step(dims), mesh=mesh,
                         in_specs=(rows_spec, P(), P(), rows_spec, rows_spec, rows_spec, vec_spec, vec_spec),
                         out_specs=(P(), P(), P()), check_vma=False)


def solution(mesh):
    nx, ny, nc = mesh.shape['col'], 4, 2
    return build(mesh, (nx, ny, mesh.shape['row'] // (ny * nc), nc))
```

```python
import functools

import jax
import jax.numpy as jnp
from jax import lax
from jax.experimental import pallas as pl
from jax.experimental.pallas import tpu as pltpu
from jax.sharding import PartitionSpec as P

F32 = jnp.float32
BF16 = jnp.bfloat16
MESH = pl.DeviceIdType.MESH
LANES = 128
PEERS = 4


def mm(a, b, ca, cb):
    return lax.dot_general(a, b, (((ca,), (cb,)), ((), ())), preferred_element_type=F32)


def split3(v):
    hi = v.astype(BF16)
    rest = v - hi.astype(F32)
    mid = rest.astype(BF16)
    low = (rest - mid.astype(F32)).astype(BF16)
    return hi, mid, low


class Grid:
    def __init__(self, dims):
        self.nx, self.ny, self.nz, self.nc = dims
        self.row = lax.axis_index('row')
        self.x = lax.axis_index('col')
        self.c = lax.rem(self.row, self.nc)
        self.y = lax.rem(self.row // self.nc, self.ny)
        self.z = self.row // (self.nc * self.ny)
        self.n_rows = self.nz * self.ny * self.nc

    def size(self, axis):
        return {'x': self.nx, 'y': self.ny, 'z': self.nz, 'c': self.nc}[axis]

    def pos(self, axis):
        return getattr(self, axis)

    def plus(self, axis, d):
        n = self.size(axis)
        return lax.rem(self.pos(axis) + d, n)

    def dev(self, axis, d):
        at = {'x': self.x, 'y': self.y, 'z': self.z, 'c': self.c}
        at[axis] = self.plus(axis, d)
        return ((at['z'] * self.ny + at['y']) * self.nc + at['c'], at['x'])

    def peer(self, p):
        if p == 0:
            return (self.row, lax.rem(self.x + self.nx - 1, self.nx))
        if p == 1:
            return (self.row, lax.rem(self.x + 1, self.nx))
        if p == 2:
            return (lax.rem(self.row + self.n_rows - 1, self.n_rows), self.x)
        return (lax.rem(self.row + 1, self.n_rows), self.x)


class Stream:
    def __init__(self, g, refs, rows):
        (self.b, self.rc, self.h, self.r1, self.p, self.r2, self.q, self.rz,
         self.f, self.ssem, self.rsem) = refs
        self.g, self.rows = g, rows
        self.n_sem = 0
        self.sent = []

    def copy(self, src, dst, dev):
        k = self.n_sem
        self.n_sem += 1
        op = pltpu.make_async_remote_copy(src_ref=src, dst_ref=dst, send_sem=self.ssem.at[k],
                                          recv_sem=self.rsem.at[k], device_id=dev, device_id_type=MESH)
        op.start()
        self.sent.append(op)
        return op

    def steps(self):
        g, rows = self.g, self.rows
        half, quarter = rows // 2, rows // 4
        ds = lambda start, size: pl.ds(pl.multiple_of(start, size), size)
        orders = (('x', 'y'), ('y', 'x'))
        other = g.plus('c', 1)
        op = self.copy(self.b.at[ds(other * half, half)], self.rc, g.dev('c', 1))
        yield
        op.wait_recv()
        self.h[...] = self.b[ds(g.c * half, half)] + self.rc[...]
        n1 = quarter // g.nx
        ops = []
        for col, (a1, a2) in enumerate(orders):
            for d in range(1, g.size(a1)):
                ops.append(self.copy(self.h.at[ds(col * quarter + g.plus(a1, d) * n1, n1)],
                                     self.r1.at[col, d - 1], g.dev(a1, d)))
        yield
        for op in ops:
            op.wait_recv()
        for col, (a1, a2) in enumerate(orders):
            total = self.h[ds(col * quarter + g.pos(a1) * n1, n1)]
            for d in range(1, g.size(a1)):
                total = total + self.r1[col, d - 1]
            self.p[col] = total
        n2 = n1 // g.ny
        ops = []
        for col, (a1, a2) in enumerate(orders):
            for d in range(1, g.size(a2)):
                ops.append(self.copy(self.p.at[col, ds(g.plus(a2, d) * n2, n2)],
                                     self.r2.at[col, d - 1], g.dev(a2, d)))
        yield
        for op in ops:
            op.wait_recv()
        for col, (a1, a2) in enumerate(orders):
            total = self.p[col, ds(g.pos(a2) * n2, n2)]
            for d in range(1, g.size(a2)):
                total = total + self.r2[col, d - 1]
            self.q[pl.ds(col * n2, n2)] = total
        n3 = 2 * n2 // g.nz
        ops = []
        for d in range(1, g.nz):
            ops.append(self.copy(self.q.at[ds(g.plus('z', d) * n3, n3)], self.rz.at[d - 1], g.dev('z', d)))
        yield
        for op in ops:
            op.wait_recv()
        total = self.q[ds(g.z * n3, n3)]
        for d in range(1, g.nz):
            total = total + self.rz[d - 1]
        base1 = [g.c * half + col * quarter for col in range(2)]
        base2 = [base1[0] + g.x * n1, base1[1] + g.y * n1]
        base3 = [base2[0] + g.y * n2, base2[1] + g.x * n2]
        per_col = g.nz // 2
        which = g.z // per_col
        start = base3[0] * (1 - which) + base3[1] * which + lax.rem(g.z, per_col) * n3
        self.f[ds(start, n3)] = total
        ops = []
        for d in range(1, g.nz):
            ops.append(self.copy(self.f.at[ds(start, n3)], self.f.at[ds(start, n3)], g.dev('z', d)))
        yield
        for op in ops:
            op.wait_recv()
        ops = []
        for col, (a1, a2) in enumerate(orders):
            for d in range(1, g.size(a2)):
                part = self.f.at[ds(base3[col], n2)]
                ops.append(self.copy(part, part, g.dev(a2, d)))
        yield
        for op in ops:
            op.wait_recv()
        ops = []
        for col, (a1, a2) in enumerate(orders):
            for d in range(1, g.size(a1)):
                part = self.f.at[ds(base2[col], n1)]
                ops.append(self.copy(part, part, g.dev(a1, d)))
        yield
        for op in ops:
            op.wait_recv()
        part = self.f.at[ds(g.c * half, half)]
        op = self.copy(part, part, g.dev('c', 1))
        yield
        op.wait_recv()
        for op in self.sent:
            op.wait_send()


def step_kernel(dims, feat_in, classes, feat_hbm, w1_hbm, w2_hbm, send_hbm, src_hbm, wt_hbm, lab_hbm, mask_hbm,
                loss_ref, g1_ref, g2_ref, *scratch):
    (feat_ref, w1_ref, w2_ref, send_ref, src_ref, wt_ref, lab_ref, mask_ref, in_sem,
     at, ath, fp, w1p, w2p, sel, z1t, z1tb, h1t, h1h, z2own, z2t, d1t, ptc,
     hs, hr, hs_sem, hr_sem, mb, mr, ms_sem, mr_sem, seen) = scratch[:32]
    refs2, refs1 = scratch[32:43], scratch[43:54]
    scope = jax.named_scope
    g = Grid(dims)
    n = feat_ref.shape[1]
    hid = w1_ref.shape[1]
    halo = send_ref.shape[0] * send_ref.shape[1]
    per = send_ref.shape[1]
    deg = src_ref.shape[0]
    ext = n + halo

    barrier = pltpu.get_barrier_semaphore()
    greet = [g.dev('c', 1)]
    for axis in ('x', 'y'):
        greet += [g.dev(axis, d) for d in range(1, g.size(axis))]
    beside = [g.dev('z', d) for d in sorted({1, g.nz - 1})]
    greet += beside
    far = lax.rem(g.row + g.n_rows + 2 * g.c - 1, g.n_rows)
    greet.append((far, g.x))
    for dev in greet:
        pl.semaphore_signal(barrier, inc=1, device_id=dev, device_id_type=MESH)

    loads = {}
    for k, (name, src, dst) in enumerate((
            ('send', send_hbm, send_ref), ('feat', feat_hbm, feat_ref), ('mask', mask_hbm, mask_ref),
            ('src', src_hbm, src_ref), ('wt', wt_hbm, wt_ref), ('w1', w1_hbm, w1_ref),
            ('lab', lab_hbm, lab_ref), ('w2', w2_hbm, w2_ref))):
        loads[name] = pltpu.make_async_copy(src, dst, in_sem.at[k])
        loads[name].start()

    def loaded(*names):
        for name in names:
            loads[name].wait()

    with scope('prep'):
        loaded('send', 'feat', 'mask')
        weight = mask_ref[...].astype(F32)
        mb[0] = jnp.full(mb.shape[1:], 1.0, F32) * jnp.sum(weight)
        eye = lax.broadcasted_iota(jnp.int32, (per, per), 0) == lax.broadcasted_iota(jnp.int32, (per, per), 1)
        lane_ids = lax.broadcasted_iota(jnp.int32, (per, n), 1)
        picks = []
        for p in range(PEERS):
            rows = jnp.broadcast_to(send_ref[p:p + 1, :], (per, per))
            column = jnp.sum(jnp.where(eye, rows, 0), axis=1, keepdims=True)
            picks.append((column == lane_ids).astype(F32))
        one_sel = jnp.concatenate(picks, axis=0).astype(BF16)
        for j in range(3):
            sel[j * halo:(j + 1) * halo, :] = one_sel
        fp[...] = jnp.concatenate([feat_ref[...].astype(F32), jnp.zeros((LANES - feat_in, n), F32)], axis=0).astype(BF16)
        first_rows = mm(one_sel, fp[...], 1, 1)

    with scope('barrier'):
        pl.semaphore_wait(barrier, len(greet))

    def exchange(stage, rows):
        hs[stage] = rows
        ops = []
        for p in range(PEERS):
            ops.append(pltpu.make_async_remote_copy(
                src_ref=hs.at[stage, pl.ds(p * per, per)], dst_ref=hr.at[stage, pl.ds((p ^ 1) * per, per)],
                send_sem=hs_sem.at[stage, p], recv_sem=hr_sem.at[stage, p ^ 1],
                device_id=g.peer(p), device_id_type=MESH))
            ops[-1].start()
        return ops

    def arrived(ops):
        for op in ops:
            op.wait()

    def count_steps():
        k = 0
        for stage, axis in enumerate(('c', 'x', 'y', 'z')):
            ops = []
            for d in range(1, g.size(axis)):
                ops.append(pltpu.make_async_remote_copy(
                    src_ref=mb.at[stage], dst_ref=mr.at[k], send_sem=ms_sem.at[k], recv_sem=mr_sem.at[k],
                    device_id=g.dev(axis, d), device_id_type=MESH))
                ops[-1].start()
                k += 1
            yield
            arrived(ops)
            total = mb[stage]
            for j in range(k - len(ops), k):
                total = total + mr[j]
            mb[stage + 1] = total

    def seen_steps():
        for rnd in range(seen.shape[0]):
            for dev in beside:
                pl.semaphore_signal(seen.at[rnd], inc=1, device_id=dev, device_id_type=MESH)
            yield
            pl.semaphore_wait(seen.at[rnd], len(beside))

    def three(stack):
        return jnp.concatenate([stack, stack, stack], axis=0)

    ops = exchange(0, first_rows)
    count = count_steps()
    next(count)
    rounds = seen_steps()
    next(rounds, None)

    with scope('build'):
        loaded('src', 'wt')

        def build(i, carry):
            first = pl.multiple_of(i * 16, 16)
            ids = first + lax.broadcasted_iota(jnp.int32, (16, n), 0)
            total = jnp.zeros((16, n), F32)
            for k in range(deg):
                total = total + jnp.where(src_ref[k:k + 1, :] == ids, wt_ref[k:k + 1, :], 0.0)
            parts = split3(total)
            for j in range(3):
                at[j, pl.ds(first, 16), :] = parts[j]
            return carry

        lax.fori_loop(0, ext // 16, build, 0)
        for j in range(3):
            ath[j * halo:(j + 1) * halo, :] = at[j, n:ext, :]

    with scope('z1own'):
        next(count)
        next(rounds, None)
        z1 = mm(fp[...], at[0, 0:n, :], 1, 0) + mm(fp[...], at[1, 0:n, :], 1, 0) + mm(fp[...], at[2, 0:n, :], 1, 0)
        loaded('w1')
        w1p[...] = jnp.concatenate([w1_ref[...], jnp.zeros((w1p.shape[0] - feat_in, hid), F32)], axis=0).astype(BF16)
    with scope('z1wait'):
        arrived(ops)
    with scope('z1'):
        z1 = z1 + mm(three(hr[0].astype(BF16)), ath[...], 0, 0)
        z1t[...] = z1.astype(BF16)
        ops = exchange(1, mm(sel[0:halo, :], z1t[...], 1, 1))
        next(rounds, None)
    kf = w1p.shape[0]
    chunk = min(hid, 512)
    n_chunks = hid // chunk
    with scope('h1'):
        for i in range(n_chunks):
            s = slice(i * chunk, (i + 1) * chunk)
            h1t[s, :] = jnp.maximum(mm(w1p[:, s], z1t[0:kf, :], 0, 0), 0.0).astype(BF16)
        z1tb[0:LANES // 2, :] = jnp.zeros((LANES // 2, n), BF16)
        z1tb[LANES // 2:, :] = z1t[0:LANES // 2, :]
        loaded('w2')
        wide = jnp.concatenate([w2_ref[...], jnp.zeros((hid, LANES - classes), F32)], axis=1).astype(BF16)
        w2p[:, 0:LANES] = wide
        w2p[:, LANES:2 * LANES] = wide
    with scope('countx'):
        next(count)

    with scope('own'):
        for i in range(n_chunks):
            s = slice(i * chunk, (i + 1) * chunk)
            z2own[s, :] = (mm(h1t[s, :], at[0, 0:n, :], 1, 0) + mm(h1t[s, :], at[1, 0:n, :], 1, 0)
                           + mm(h1t[s, :], at[2, 0:n, :], 1, 0))
            if i == 0:
                for _ in rounds:
                    pass
                next(count)
    with scope('z2wait'):
        arrived(ops)
    with scope('z2'):
        z1h = three(hr[1][:, 0:kf].astype(BF16))
        logits = jnp.zeros((LANES, n), F32)
        for i in range(n_chunks):
            s = slice(i * chunk, (i + 1) * chunk)
            h1h[s, :] = jnp.maximum(mm(w1p[:, s], z1h, 0, 1), 0.0).astype(BF16)
            z2 = (z2own[s, :] + mm(h1h[s, :], ath[...], 1, 0)).astype(BF16)
            z2t[s, :] = z2
            logits = logits + mm(w2p[s, 0:LANES], z2, 0, 0)
    with scope('countwait'):
        for _ in count:
            pass

    with scope('softmax'):
        loaded('lab')
        label_count = mb[4, 0:1, 0:1]
        ids = lax.broadcasted_iota(jnp.int32, (LANES, n), 0)
        valid = ids < classes
        top = jnp.max(jnp.where(valid, logits, -jnp.inf), axis=0, keepdims=True)
        log_norm = jnp.log(jnp.sum(jnp.where(valid, jnp.exp(logits - top), 0.0), axis=0, keepdims=True)) + top
        onehot = ids == lab_ref[...]
        picked = jnp.sum(jnp.where(onehot, logits, 0.0), axis=0, keepdims=True)
        loss = jnp.sum(weight * (log_norm - picked))
        prob = jnp.exp(logits - log_norm)
        scale = weight / label_count
        gt = jnp.where(valid, (prob - onehot.astype(F32)) * scale, 0.0).astype(BF16)
        back = mm(ath[...], gt, 1, 1)
        ops = exchange(2, back[0:halo] + back[halo:2 * halo] + back[2 * halo:3 * halo])

    with scope('grad2'):
        b2 = refs2[0]
        lane = lax.broadcasted_iota(jnp.int32, (chunk, LANES), 1)
        for i in range(n_chunks):
            s = slice(i * chunk, (i + 1) * chunk)
            b2[s, :] = jnp.where(lane == classes, loss, mm(z2t[s, :], gt, 1, 1))
        stream2 = Stream(g, refs2, hid).steps()
        next(stream2)

    with scope('ptown'):
        pt = mm(gt, at[0, 0:n, :], 1, 1) + mm(gt, at[1, 0:n, :], 1, 1) + mm(gt, at[2, 0:n, :], 1, 1)
    with scope('s2core'):
        next(stream2)
    with scope('ptwait'):
        arrived(ops)
    with scope('dh'):
        pt = pt + mm(jnp.concatenate(split3(hr[2]), axis=0), sel[...], 0, 0)
        for j, part in enumerate(split3(pt)):
            ptc[j * LANES:(j + 1) * LANES, :] = part
        for i in range(n_chunks):
            s = slice(i * chunk, (i + 1) * chunk)
            dh = mm(w2p[s, :], ptc[0:2 * LANES, :], 1, 0) + mm(w2p[s, 0:LANES], ptc[2 * LANES:3 * LANES, :], 1, 0)
            d1t[s, :] = jnp.where(h1t[s, :].astype(F32) > 0.0, dh, 0.0).astype(BF16)
    with scope('grad1'):
        b1 = refs1[0]
        half = hid // 2
        b1[...] = mm(d1t[0:half, :], z1t[...], 1, 1) + mm(d1t[half:hid, :], z1tb[...], 1, 1)
        stream1 = Stream(g, refs1, half).steps()
        next(stream1)
    active = [(2, stream2), (1, stream1)]
    k = 0
    while active:
        for which, stream in list(active):
            k += 1
            with scope('sum%d_%d' % (which, k)):
                if next(stream, 'end') == 'end':
                    active.remove((which, stream))

    with scope('out'):
        f2, f1 = refs2[8], refs1[8]
        loss_ref[...] = f2[0:1, classes:classes + 1] / label_count
        g2_ref[...] = f2[:, 0:classes]
        flip = jnp.transpose(f1[...])
        g1_ref[:, 0:half] = flip[0:feat_in, :]
        g1_ref[:, half:hid] = flip[LANES // 2:LANES // 2 + feat_in, :]


def stream_scratch(rows, dims):
    nx, ny, nz, nc = dims
    half, quarter = rows // 2, rows // 4
    n1 = quarter // nx
    n2 = n1 // ny
    n3 = 2 * n2 // nz
    copies = 2 + 4 * (nx - 1) + 4 * (ny - 1) + 2 * (nz - 1)
    return [
        pltpu.VMEM((rows, LANES), F32), pltpu.VMEM((half, LANES), F32), pltpu.VMEM((half, LANES), F32),
        pltpu.VMEM((2, nx - 1, n1, LANES), F32), pltpu.VMEM((2, n1, LANES), F32),
        pltpu.VMEM((2, ny - 1, n2, LANES), F32), pltpu.VMEM((2 * n2, LANES), F32),
        pltpu.VMEM((nz - 1, n3, LANES), F32), pltpu.VMEM((rows, LANES), F32),
        pltpu.SemaphoreType.DMA((copies,)), pltpu.SemaphoreType.DMA((copies,))]


def make_step(dims):
    def device_step(node_feat, w_one, w_two, send_rows, edge_src, edge_wt, labels, label_mask):
        n, feat_in = node_feat.shape
        hid, classes = w_two.shape
        halo = send_rows.size
        ext = n + halo
        deg = edge_src.shape[1]
        nx, ny, nz, nc = dims
        n_count = nx + ny + nz + nc - 4
        kf = 64
        scratch = [
            pltpu.VMEM((feat_in, n), BF16), pltpu.VMEM((feat_in, hid), F32), pltpu.VMEM((hid, classes), F32),
            pltpu.VMEM(send_rows.shape, jnp.int32), pltpu.VMEM((deg, n), jnp.int32), pltpu.VMEM((deg, n), F32),
            pltpu.VMEM((1, n), jnp.int32), pltpu.VMEM((1, n), jnp.int32), pltpu.SemaphoreType.DMA((8,)),
            pltpu.VMEM((3, ext, n), BF16), pltpu.VMEM((3 * halo, n), BF16), pltpu.VMEM((LANES, n), BF16),
            pltpu.VMEM((kf, hid), BF16), pltpu.VMEM((hid, 2 * LANES), BF16), pltpu.VMEM((3 * halo, n), BF16),
            pltpu.VMEM((LANES, n), BF16), pltpu.VMEM((LANES, n), BF16),
            pltpu.VMEM((hid, n), BF16), pltpu.VMEM((hid, 3 * halo), BF16), pltpu.VMEM((hid, n), F32),
            pltpu.VMEM((hid, n), BF16), pltpu.VMEM((hid, n), BF16), pltpu.VMEM((3 * LANES, n), BF16),
            pltpu.VMEM((3, halo, LANES), F32), pltpu.VMEM((3, halo, LANES), F32),
            pltpu.SemaphoreType.DMA((3, PEERS)), pltpu.SemaphoreType.DMA((3, PEERS)),
            pltpu.VMEM((5, 8, LANES), F32), pltpu.VMEM((n_count, 8, LANES), F32),
            pltpu.SemaphoreType.DMA((n_count,)), pltpu.SemaphoreType.DMA((n_count,)),
            pltpu.SemaphoreType.REGULAR((max(nz // 2 - 1, 1),)),
        ] + stream_scratch(hid, dims) + stream_scratch(hid // 2, dims)
        vmem = pl.BlockSpec(memory_space=pltpu.VMEM)
        loss, grad_one, grad_two = pl.pallas_call(
            functools.partial(step_kernel, dims, feat_in, classes),
            out_shape=(jax.ShapeDtypeStruct((1, 1), F32), jax.ShapeDtypeStruct((feat_in, hid), F32),
                       jax.ShapeDtypeStruct((hid, classes), F32)),
            in_specs=[pl.BlockSpec(memory_space=pltpu.HBM)] * 8, out_specs=(vmem,) * 3, scratch_shapes=scratch,
            compiler_params=pltpu.CompilerParams(collective_id=0, has_side_effects=True,
                                                 vmem_limit_bytes=32 * 1024 * 1024),
        )(*[pltpu.with_memory_space_constraint(v, pltpu.HBM) for v in (
            node_feat.T, w_one, w_two, send_rows, edge_src.T, edge_wt.T, labels.reshape(1, n), label_mask.reshape(1, n))])
        return loss[0, 0], grad_one, grad_two
    return device_step


def build(mesh, dims):
    grid_axes = ('row', 'col')
    rows_spec = P(grid_axes, None)
    vec_spec = P(grid_axes)
    return jax.shard_map(make_step(dims), mesh=mesh,
                         in_specs=(rows_spec, P(), P(), rows_spec, rows_spec, rows_spec, vec_spec, vec_spec),
                         out_specs=(P(), P(), P()), check_vma=False)


def solution(mesh):
    nx, ny, nc = mesh.shape['col'], 4, 2
    return build(mesh, (nx, ny, mesh.shape['row'] // (ny * nc), nc))
```
